32 devices in a mesh: ta: 1, gx: 8 (over y, x, core), gy: 4 (over z).
Axes of the slice: x: 2, y: 2, z: 4, core: 2. Of those that a mesh axis runs over, the one named last changes fastest.
Arguments:
- propagator: bfloat16 [1, 2, 4, 3, 4, 3, 64, 4096], P('ta', None, None, None, None, None, 'gx', 'gy'), may hold values from -1.5 to 1.5
- gamma_table: int32 [16, 8], replicated, may hold values from 0 to 3, as said below
Outputs:
- spectrum: float32 [1, 16, 64, 64, 128], P('ta', None, ('gx', 'gy'))
The draws below stay inside these ranges and needn't reach their ends.
Inputs may be any that keep to these rules, and one draw needn't show every extreme that they name: gamma_table[g, 0:4] is a permutation of 0 to 3, gamma_table[g, 4:8] are powers of i.
All inputs are finite; a program needn't handle non-finite values.
Results may differ from the reference program's by a relative error of at most 0.0061.
Values may be sent and summed in bfloat16 or wider, within the bound.
A program may use at most 192 MiB of HBM per device.

```python
import math
import jax
import jax.numpy as jnp
from jax import lax

EXTENT = 64
CHANNELS = 16
SLICES = 1


def draw_gamma_table(key, part):
    subkeys = jax.random.split(key, CHANNELS)
    orders = jax.vmap(lambda subkey: jax.random.permutation(subkey, 4))(subkeys)
    phase_codes = jax.random.randint(jax.random.fold_in(key, 11), (CHANNELS, 4), 0, 4, dtype=jnp.int32)
    return jnp.concatenate([orders.astype(jnp.int32), phase_codes], axis=1)


def level_of(stream_key, extent, cuts, low, high):
    factor_of, own = 1.0, jax.random.fold_in(stream_key, 6)
    for position, blocks in cuts:
        steps = jnp.exp(jax.random.uniform(jax.random.fold_in(own, position), (blocks,), jnp.float32, low / len(cuts), high / len(cuts)))
        factor_of = factor_of * jnp.repeat(steps, extent[position] // blocks).reshape([-1 if axis == position else 1 for axis in range(len(extent))])
    return factor_of


def bell_draw(key, shape, deviation, reach, pieces=(), kind=jnp.bfloat16):
    factor_of = level_of(key, shape, pieces, -0.22, 0.18) if pieces else 1.0
    array = jax.random.normal(key, shape, jnp.float32) * deviation * factor_of
    return jnp.minimum(jnp.maximum(array, -reach), reach).astype(kind)


def setup_inputs(seed: int = 0) -> dict:
    key_of = jax.random.split(jax.random.key(seed), 3)
    propagator = bell_draw(key_of[0], (SLICES, 2, 4, 3, 4, 3, EXTENT, EXTENT * EXTENT), 0.25, 1.5, ((6, 8), (7, 4)))
    gamma_table = draw_gamma_table(jax.random.fold_in(key_of[2], 71), 0)
    return dict(propagator=propagator, gamma_table=gamma_table)


def precise_dot(left_matrix, right_matrix):
    return jnp.dot(left_matrix, right_matrix, precision=lax.Precision.HIGHEST, preferred_element_type=jnp.float32)

def channel_weights(channel_table):
    spin_index = jnp.arange(4, dtype=jnp.int32)
    targets = channel_table[:, :4]
    codes_all = channel_table[:, 4:]
    mapping = (targets[:, :, None] == spin_index[None, None, :]).astype(jnp.float32)
    phase_real = (codes_all == 0).astype(jnp.float32) - (codes_all == 2).astype(jnp.float32)
    phase_imag = (codes_all == 1).astype(jnp.float32) - (codes_all == 3).astype(jnp.float32)
    pair_real = phase_real[:, None, :] * phase_real[:, :, None] - phase_imag[:, None, :] * phase_imag[:, :, None]
    pair_imag = phase_real[:, None, :] * phase_imag[:, :, None] + phase_imag[:, None, :] * phase_real[:, :, None]
    source_map = jnp.transpose(mapping, (0, 2, 1))
    selector = source_map[:, :, None, :, None] * mapping[:, None, :, None, :]
    count_channels = channel_table.shape[0]
    weight_real = (pair_real[:, None, :, :, None] * selector).reshape(count_channels, 256)
    weight_imag = (pair_imag[:, None, :, :, None] * selector).reshape(count_channels, 256)
    return (weight_real, weight_imag)

def spin_products(field_real, field_imag):
    site_count = field_real.shape[-1]
    total_real = jnp.zeros((4, 4, 4, 4, site_count), jnp.float32)
    total_imag = jnp.zeros((4, 4, 4, 4, site_count), jnp.float32)
    for color_in in range(3):
        for color_out in range(3):
            left_real = field_real[:, color_in, :, color_out].astype(jnp.float32)
            left_imag = field_imag[:, color_in, :, color_out].astype(jnp.float32)
            total_real = total_real + left_real[:, :, None, None] * left_real[None, None] + left_imag[:, :, None, None] * left_imag[None, None]
            total_imag = total_imag + left_imag[:, :, None, None] * left_real[None, None] - left_real[:, :, None, None] * left_imag[None, None]
    return (total_real.reshape(256, site_count), total_imag.reshape(256, site_count))

def dft_tables(length):
    steps_index = jnp.arange(length, dtype=jnp.int32)
    phases = steps_index[:, None] * steps_index[None, :] % length
    angles = phases.astype(jnp.float32) * (2.0 * math.pi / length)
    norm_factor = 1.0 / math.sqrt(length)
    cosine = (jnp.cos(angles) * norm_factor).astype(jnp.bfloat16)
    sine_table = (jnp.sin(angles) * norm_factor).astype(jnp.bfloat16)
    return (cosine.astype(jnp.float32), sine_table.astype(jnp.float32))

def section(complex_pair, which_axis, cosine, sine_table):
    field_real = complex_pair[0].astype(jnp.float32)
    field_imag = complex_pair[1].astype(jnp.float32)

    def contract_axis(values, weights):
        moved = jnp.tensordot(values, weights, axes=([which_axis], [0]), precision=lax.Precision.HIGHEST)
        return jnp.moveaxis(moved, -1, which_axis)
    new_real = contract_axis(field_real, cosine) + contract_axis(field_imag, sine_table)
    new_imag = contract_axis(field_imag, cosine) - contract_axis(field_real, sine_table)
    return (new_real, new_imag)

def to_half(complex_pair):
    return lax.optimization_barrier((complex_pair[0].astype(jnp.bfloat16), complex_pair[1].astype(jnp.bfloat16)))

def reference(propagator, gamma_table):
    weight_real, weight_imag = channel_weights(gamma_table)
    stack_real = jnp.concatenate([weight_real, -weight_imag], axis=1)
    stack_imag = jnp.concatenate([weight_imag, weight_real], axis=1)
    cosine, sine_table = dft_tables(EXTENT)
    volume = EXTENT ** 3

    def one_slice(slice_block):
        flattened = slice_block.astype(jnp.float32).reshape(2, 4, 3, 4, 3, volume)
        prod_real, prod_imag = spin_products(flattened[0], flattened[1])
        prod_stack = jnp.concatenate([prod_real, prod_imag], axis=0).astype(jnp.bfloat16)
        prod_stack = lax.optimization_barrier(prod_stack).astype(jnp.float32)
        dens_real = precise_dot(stack_real, prod_stack).reshape(-1, EXTENT, EXTENT, EXTENT)
        dens_imag = precise_dot(stack_imag, prod_stack).reshape(-1, EXTENT, EXTENT, EXTENT)
        pair = to_half((dens_real, dens_imag))
        pair = to_half(section(pair, 3, cosine, sine_table))
        pair = to_half(section(pair, 2, cosine, sine_table))
        spec_real, spec_imag = section(pair, 1, cosine, sine_table)
        spec_real = jnp.transpose(spec_real, (0, 3, 1, 2))
        spec_imag = jnp.transpose(spec_imag, (0, 3, 1, 2))
        return jnp.concatenate([spec_real, spec_imag], axis=3).astype(jnp.float32)
    return lax.map(one_slice, propagator)
```

```python
import functools
import math

import jax
import jax.numpy as jnp
import numpy as np
from jax import lax
from jax.experimental import pallas as pl
from jax.experimental.pallas import tpu as pltpu
from jax.sharding import PartitionSpec as P

LANES = 128
SPINS = 4
COLORS = 3
PITCH = 8
PAIRED = 2
MESH = pl.DeviceIdType.MESH


def pair_rows():
    rows = []
    for left in range(SPINS):
        for right in range(left, SPINS):
            for i in range(SPINS):
                for j in range(SPINS):
                    if left == right and i > j:
                        continue
                    if left == right and i == j:
                        rows.append((left, i, right, j, 2))
                    else:
                        rows.append((left, i, right, j, 0))
                        rows.append((left, i, right, j, 1))
    return rows


ROWS = pair_rows()
ROW_OF = {row: position for position, row in enumerate(ROWS)}


def dft_tables(length):
    index = np.arange(length)
    angles = (index[:, None] * index[None, :] % length) * (2.0 * math.pi / length)
    norm = 1.0 / math.sqrt(length)
    half = lambda v: (v * norm).astype(jnp.bfloat16).astype(np.float32)
    return half(np.cos(angles)), half(np.sin(angles))


def table_z(extent):
    cosine, sine = dft_tables(extent)
    per_tile = LANES // extent
    same = np.eye(per_tile, dtype=np.float32)
    block = np.zeros((extent, 2, per_tile, 2, per_tile, extent), np.float32)
    for c_out, c_in, values in ((0, 0, cosine), (0, 1, sine), (1, 0, -sine), (1, 1, cosine)):
        block[:, c_out, :, c_in] = np.einsum("zk,ab->kabz", values, same)
    return block.reshape(2 * LANES, 2 * LANES)


def table_y(extent, local_k):
    cosine, sine = dft_tables(extent)
    per_tile = LANES // extent
    groups = extent // per_tile
    block = np.zeros((groups, local_k, 2, per_tile, 2, local_k, 2, extent), np.float32)
    entries = (
        (0, 0, 0, cosine), (0, 0, 1, sine), (0, 1, 0, -sine), (0, 1, 1, cosine),
        (1, 0, 0, -sine), (1, 0, 1, cosine), (1, 1, 0, -cosine), (1, 1, 1, -sine),
    )
    for copy, c_out, c_in, values in entries:
        for k in range(local_k):
            block[:, k, c_in, :, copy, k, c_out] = values.reshape(groups, per_tile, extent)
    return block.reshape(groups * local_k * 2 * per_tile, 2 * local_k * 2 * extent)


def table_x(extent):
    cosine, sine = dft_tables(extent)
    return np.concatenate([cosine.T, sine.T], axis=1)


def folded_weights(table, rows):
    channels = table.shape[0]
    a1, a2, b1, b2, kind = (rows[i : i + 1, :] for i in range(5))

    def pick(spin, base):
        value = jnp.zeros((channels, rows.shape[1]), jnp.int32)
        for s in range(SPINS):
            value = jnp.where(spin == s, table[:, base + s : base + s + 1], value)
        return value

    def term(l1, l2, r1, r2):
        hit = (pick(r1, 0) == l1) & (pick(l2, 0) == r2)
        code = (pick(r1, SPINS) + pick(l2, SPINS)) & 3
        one = jnp.where(hit, 1.0, 0.0)
        real = jnp.where(code == 0, one, jnp.where(code == 2, -one, 0.0))
        imag = jnp.where(code == 1, one, jnp.where(code == 3, -one, 0.0))
        return real, imag

    fore_real, fore_imag = term(a1, a2, b1, b2)
    back_real, back_imag = term(b1, b2, a1, a2)
    sign = jnp.where(kind == 0, 1.0, jnp.where(kind == 1, -1.0, 0.0))
    real = fore_real + sign * back_real
    imag = fore_imag + sign * back_imag
    weight_real = jnp.where(kind == 1, -imag, real)
    weight_imag = jnp.where(kind == 1, real, imag)
    return jnp.concatenate([weight_real, weight_imag], axis=0).astype(jnp.bfloat16)


def component(s1, c1, s2, c2):
    return ((s1 * COLORS + c1) * SPINS + s2) * COLORS + c2


def products(parts, rows_out):
    entries = parts.shape[0] // 2
    pitch = rows_out.shape[1] // parts.shape[1]

    def put(row, value):
        value = value.astype(jnp.float32)
        for h in range(PAIRED):
            rows_out[h, pl.ds(ROW_OF[row], parts.shape[1], stride=pitch), :] = (
                value[:, h * LANES : (h + 1) * LANES]
            )

    def group(terms):
        total = terms[0]
        for term in terms[1:]:
            total = total + term
        return total

    for left in range(SPINS):
        for right in range(left, SPINS):
            for half in ((0, 1), (2, 3)):
                pairs = [(i, j) for i in half for j in range(SPINS) if left != right or i < j]
                diagonal = half if left == right else ()
                sums = {}
                for c1 in range(COLORS):
                    part = {}
                    for c2 in range(COLORS):
                        at_a = {i: component(left, c1, i, c2) for i in half}
                        at_b = {j: component(right, c1, j, c2) for j in sorted({j for _, j in pairs})}
                        a = {i: (parts[n], parts[entries + n]) for i, n in at_a.items()}
                        b = {j: (parts[n], parts[entries + n]) for j, n in at_b.items()}
                        for i, j in pairs:
                            re = a[i][0] * b[j][0] + a[i][1] * b[j][1]
                            im = a[i][1] * b[j][0] - a[i][0] * b[j][1]
                            old = part.get((i, j))
                            part[i, j] = (re, im) if old is None else (old[0] + re, old[1] + im)
                        for i in diagonal:
                            re = a[i][0] * a[i][0] + a[i][1] * a[i][1]
                            old = part.get(i)
                            part[i] = (re,) if old is None else (old[0] + re,)
                    for key, values in part.items():
                        values = tuple(v.astype(jnp.float32) for v in values)
                        old = sums.get(key)
                        sums[key] = values if old is None else tuple(o + v for o, v in zip(old, values))
                for i, j in pairs:
                    put((left, i, right, j, 0), sums[i, j][0])
                    put((left, i, right, j, 1), sums[i, j][1])
                for i in diagonal:
                    put((left, i, right, i, 2), sums[i][0])


def front_kernel(
    grid_x, grid_y, prop, table_in, rows_in, dft_in, out,
    staged, prod, dens, weights, sent, table, rows, dft,
    load_sems, small_sems, send_sem, recv_sem,
):
    devices = out.shape[0]
    tiles = staged.shape[0]
    rows_x, width = staged.shape[2:]
    pitch = prod.shape[1] // rows_x
    channels = table.shape[1]

    def load(t):
        return pltpu.make_async_copy(
            prop.at[:, :, pl.ds(t * width, width)], staged.at[t], load_sems.at[t]
        )

    me_x, me_y = lax.axis_index("gx"), lax.axis_index("gy")
    me = me_x * grid_y + me_y
    if grid_y == 4:
        low = lax.rem(me_y, 2)
        other = 2 - (me_y - low)
        far, near = [other + low, other + 1 - low], [me_y + 1 - 2 * low]
    else:
        far, near = [lax.rem(me_y + i, grid_y) for i in range(1, grid_y)], []

    def for_others(act):
        @pl.loop(0, grid_x)
        def _(i):
            to_x = lax.rem(me_x + i, grid_x)
            for to_y in far:
                act(to_x, to_y)

        @pl.loop(1, grid_x)
        def _(i):
            to_x = lax.rem(me_x + i, grid_x)
            for to_y in near:
                act(to_x, to_y)
            act(to_x, me_y)

        for to_y in near:
            act(me_x, to_y)

    small = [
        pltpu.make_async_copy(source, target, small_sems.at[n])
        for n, (source, target) in enumerate(((table_in, table), (rows_in, rows), (dft_in, dft)))
    ]
    load(0).start()
    for copy in small:
        copy.start()
    for t in range(1, tiles):
        load(t).start()
    barrier = pltpu.get_barrier_semaphore()
    for_others(
        lambda x, y: pl.semaphore_signal(
            barrier, inc=1, device_id={"gx": x, "gy": y}, device_id_type=MESH
        )
    )
    small[0].wait()
    small[1].wait()
    weights[...] = folded_weights(jnp.transpose(table[...]), rows[...])
    small[2].wait()

    @pl.loop(0, tiles)
    def _(t):
        load(t).wait()
        products(staged.at[t], prod)
        for h in range(PAIRED):
            for x in range(rows_x):
                columns = prod[h, pl.ds(x * pitch, len(ROWS)), :].astype(jnp.bfloat16)
                value = jnp.dot(weights[...], columns, preferred_element_type=jnp.float32)
                dens[h, 0, pl.ds(x, channels, stride=rows_x), :] = value[:channels]
                dens[h, 1, pl.ds(x, channels, stride=rows_x), :] = value[channels:]
        left = jnp.concatenate(
            [jnp.concatenate([dens[h, 0], dens[h, 1]], axis=1) for h in range(PAIRED)], axis=0
        ).astype(jnp.bfloat16)
        value = lax.dot_general(
            dft[...], left, (((1,), (1,)), ((), ())), preferred_element_type=jnp.float32
        )
        pieces = [
            value[:, h * LANES : (h + 1) * LANES].reshape(devices, 2 * LANES // devices, LANES)
            for h in range(PAIRED)
        ]
        sent[:, t] = jnp.concatenate(pieces, axis=1).astype(jnp.bfloat16)
        out[me, t] = sent[me, t]

        @pl.when(t == 0)
        def _():
            pl.semaphore_wait(barrier, grid_x * grid_y - 1)

        for_others(
            lambda x, y: pltpu.make_async_remote_copy(
                src_ref=sent.at[x * grid_y + y, t], dst_ref=out.at[me, t],
                send_sem=send_sem, recv_sem=recv_sem,
                device_id={"gx": x, "gy": y}, device_id_type=MESH,
            ).start()
        )

    rest = sent.at[pl.ds(0, devices - 1)]
    pltpu.make_async_copy(rest, rest, recv_sem).wait()
    pltpu.make_async_copy(rest, rest, send_sem).wait()


def front(prop, gamma_table, devices, grid_y, extent):
    entries, rows_x, sites = prop.shape
    tiles = sites // (LANES * PAIRED)
    height = 2 * LANES // devices * PAIRED
    channels = gamma_table.shape[0]
    rows = np.zeros((8, len(ROWS)), np.int32)
    rows[:5] = np.array(ROWS, np.int32).T
    pinned = [
        pltpu.with_memory_space_constraint(array, pltpu.HBM)
        for array in (
            prop, gamma_table.T, jnp.asarray(rows), jnp.asarray(table_z(extent), jnp.bfloat16)
        )
    ]
    return pl.pallas_call(
        functools.partial(front_kernel, devices // grid_y, grid_y),
        out_shape=pltpu.VMEM((devices, tiles, height, LANES), jnp.bfloat16),
        in_specs=[pl.BlockSpec(memory_space=pltpu.HBM)] * 4,
        out_specs=pl.BlockSpec(memory_space=pltpu.VMEM),
        scratch_shapes=[
            pltpu.VMEM((tiles, entries, rows_x, PAIRED * LANES), jnp.bfloat16),
            pltpu.VMEM((PAIRED, (len(ROWS) + PITCH) * rows_x, LANES), jnp.float32),
            pltpu.VMEM((PAIRED, 2, channels * rows_x, LANES), jnp.float32),
            pltpu.VMEM((2 * channels, len(ROWS)), jnp.bfloat16),
            pltpu.VMEM((devices, tiles, height, LANES), jnp.bfloat16),
            pltpu.VMEM(gamma_table.shape[::-1], jnp.int32),
            pltpu.VMEM(rows.shape, jnp.int32),
            pltpu.VMEM((2 * LANES, 2 * LANES), jnp.bfloat16),
            pltpu.SemaphoreType.DMA((tiles,)),
            pltpu.SemaphoreType.DMA((3,)),
            pltpu.SemaphoreType.DMA,
            pltpu.SemaphoreType.DMA,
        ],
        compiler_params=pltpu.CompilerParams(
            vmem_limit_bytes=60 * 1024 * 1024, collective_id=0, has_side_effects=True
        ),
    )(*pinned)


def back_kernel(blocks, along_y, along_x, out, mid):
    grid_x, _, width = blocks.shape
    channels, local_k, extent, lanes = out.shape
    rows_x = width // channels
    cols = local_k * lanes
    for gx in range(grid_x):
        mid[gx] = lax.dot_general(
            blocks[gx], along_y[...], (((0,), (0,)), ((), ())), preferred_element_type=jnp.float32
        )
    for g in range(channels):
        value = mid[:, g * rows_x : (g + 1) * rows_x, :].reshape(grid_x * rows_x, 2 * cols)
        value = value.astype(jnp.bfloat16)
        stacked = jnp.concatenate([value[:, :cols], value[:, cols:]], axis=0)
        result = jnp.dot(along_x[...], stacked, preferred_element_type=jnp.float32)
        for k in range(local_k):
            out[g, k] = result[:, k * lanes : (k + 1) * lanes]


def back(blocks, channels, extent, local_k):
    grid_x, _, width = blocks.shape
    vmem = pl.BlockSpec(memory_space=pltpu.VMEM)
    return pl.pallas_call(
        back_kernel,
        out_shape=jax.ShapeDtypeStruct((channels, local_k, extent, 2 * extent), jnp.float32),
        in_specs=[vmem] * 3,
        out_specs=vmem,
        scratch_shapes=[pltpu.VMEM((grid_x, width, 4 * local_k * extent), jnp.float32)],
        compiler_params=pltpu.CompilerParams(vmem_limit_bytes=24 * 1024 * 1024),
    )(
        blocks,
        jnp.asarray(table_y(extent, local_k), jnp.bfloat16),
        jnp.asarray(table_x(extent), jnp.bfloat16),
    )


def body(propagator, gamma_table):
    slices, rows_x, sites = propagator.shape[0], propagator.shape[-2], propagator.shape[-1]
    grid_x, grid_y = lax.axis_size("gx"), lax.axis_size("gy")
    devices = grid_x * grid_y
    extent = grid_x * rows_x
    channels = gamma_table.shape[0]
    local_k = extent // devices
    results = []
    for t in range(slices):
        prop = propagator[t].reshape(-1, rows_x, sites)
        blocks = front(prop, gamma_table, devices, grid_y, extent)
        blocks = blocks.reshape(grid_x, -1, LANES)
        results.append(back(blocks, channels, extent, local_k))
    return jnp.stack(results)


def solution(mesh):
    return jax.shard_map(
        body,
        mesh=mesh,
        in_specs=(P("ta", None, None, None, None, None, "gx", "gy"), P()),
        out_specs=P("ta", None, ("gx", "gy"), None, None),
        check_vma=False,
    )
```

```python
import functools
import math

import jax
import jax.numpy as jnp
import numpy as np
from jax import lax
from jax.experimental import pallas as pl
from jax.experimental.pallas import tpu as pltpu
from jax.sharding import PartitionSpec as P

LANES = 128
SPINS = 4
COLORS = 3
PITCH = 8
PAIRED = 2
MESH = pl.DeviceIdType.MESH


def pair_rows():
    rows = []
    for left in range(SPINS):
        for right in range(left, SPINS):
            for i in range(SPINS):
                for j in range(SPINS):
                    if left == right and i > j:
                        continue
                    if left == right and i == j:
                        rows.append((left, i, right, j, 2))
                    else:
                        rows.append((left, i, right, j, 0))
                        rows.append((left, i, right, j, 1))
    return rows


ROWS = pair_rows()
ROW_OF = {row: position for position, row in enumerate(ROWS)}


def dft_tables(length):
    index = np.arange(length)
    angles = (index[:, None] * index[None, :] % length) * (2.0 * math.pi / length)
    norm = 1.0 / math.sqrt(length)
    half = lambda v: (v * norm).astype(jnp.bfloat16).astype(np.float32)
    return half(np.cos(angles)), half(np.sin(angles))


def table_z(extent):
    cosine, sine = dft_tables(extent)
    per_tile = LANES // extent
    same = np.eye(per_tile, dtype=np.float32)
    block = np.zeros((extent, 2, per_tile, 2, per_tile, extent), np.float32)
    for c_out, c_in, values in ((0, 0, cosine), (0, 1, sine), (1, 0, -sine), (1, 1, cosine)):
        block[:, c_out, :, c_in] = np.einsum("zk,ab->kabz", values, same)
    return block.reshape(2 * LANES, 2 * LANES)


def table_y(extent, local_k):
    cosine, sine = dft_tables(extent)
    per_tile = LANES // extent
    groups = extent // per_tile
    block = np.zeros((groups, local_k, 2, per_tile, 2, local_k, 2, extent), np.float32)
    entries = (
        (0, 0, 0, cosine), (0, 0, 1, sine), (0, 1, 0, -sine), (0, 1, 1, cosine),
        (1, 0, 0, -sine), (1, 0, 1, cosine), (1, 1, 0, -cosine), (1, 1, 1, -sine),
    )
    for copy, c_out, c_in, values in entries:
        for k in range(local_k):
            block[:, k, c_in, :, copy, k, c_out] = values.reshape(groups, per_tile, extent)
    return block.reshape(groups * local_k * 2 * per_tile, 2 * local_k * 2 * extent)


def table_x(extent):
    cosine, sine = dft_tables(extent)
    return np.concatenate([cosine.T, sine.T], axis=1)


def folded_weights(table, rows):
    channels = table.shape[0]
    a1, a2, b1, b2, kind = (rows[i : i + 1, :] for i in range(5))

    def pick(spin, base):
        value = jnp.zeros((channels, rows.shape[1]), jnp.int32)
        for s in range(SPINS):
            value = jnp.where(spin == s, table[:, base + s : base + s + 1], value)
        return value

    def term(l1, l2, r1, r2):
        hit = (pick(r1, 0) == l1) & (pick(l2, 0) == r2)
        code = (pick(r1, SPINS) + pick(l2, SPINS)) & 3
        one = jnp.where(hit, 1.0, 0.0)
        real = jnp.where(code == 0, one, jnp.where(code == 2, -one, 0.0))
        imag = jnp.where(code == 1, one, jnp.where(code == 3, -one, 0.0))
        return real, imag

    fore_real, fore_imag = term(a1, a2, b1, b2)
    back_real, back_imag = term(b1, b2, a1, a2)
    sign = jnp.where(kind == 0, 1.0, jnp.where(kind == 1, -1.0, 0.0))
    real = fore_real + sign * back_real
    imag = fore_imag + sign * back_imag
    weight_real = jnp.where(kind == 1, -imag, real)
    weight_imag = jnp.where(kind == 1, real, imag)
    return jnp.concatenate([weight_real, weight_imag], axis=0).astype(jnp.bfloat16)


def component(s1, c1, s2, c2):
    return s1, (c1 * SPINS + s2) * COLORS + c2


def products(parts, first, last, rows_out, ready=None):
    rows_x = parts.shape[-2]
    pitch = rows_out.shape[1] // rows_x

    def put(row, value):
        value = value.astype(jnp.float32)
        place = pl.ds(ROW_OF[row] - first, rows_x, stride=pitch)
        for h in range(PAIRED):
            rows_out[h, place, :] = value[:, h * LANES : (h + 1) * LANES]

    for left in range(SPINS):
        for right in range(left, SPINS):
            at = [position for row, position in ROW_OF.items() if row[::2][:2] == (left, right)]
            if not first <= at[0] < last:
                continue
            if ready and left == 0:
                ready(right)
            for half in ((0, 1), (2, 3)):
                pairs = [(i, j) for i in half for j in range(SPINS) if left != right or i < j]
                diagonal = half if left == right else ()
                sums = {}
                for c1 in range(COLORS):
                    part = {}
                    for c2 in range(COLORS):
                        at_a = {i: component(left, c1, i, c2) for i in half}
                        at_b = {j: component(right, c1, j, c2) for _, j in pairs}
                        a = {i: (parts[0, *n], parts[1, *n]) for i, n in at_a.items()}
                        b = {j: (parts[0, *n], parts[1, *n]) for j, n in at_b.items()}
                        for i, j in pairs:
                            re = a[i][0] * b[j][0] + a[i][1] * b[j][1]
                            im = a[i][1] * b[j][0] - a[i][0] * b[j][1]
                            old = part.get((i, j))
                            part[i, j] = (re, im) if old is None else (old[0] + re, old[1] + im)
                        for i in diagonal:
                            wide = tuple(v.astype(jnp.float32) for v in a[i])
                            re = wide[0] * wide[0] + wide[1] * wide[1]
                            old = part.get(i)
                            part[i] = (re,) if old is None else (old[0] + re,)
                    for key, values in part.items():
                        old = sums.get(key)
                        sums[key] = values if old is None else tuple(o + v for o, v in zip(old, values))
                for i, j in pairs:
                    put((left, i, right, j, 0), sums[i, j][0])
                    put((left, i, right, j, 1), sums[i, j][1])
                for i in diagonal:
                    put((left, i, right, i, 2), sums[i][0])


def front_kernel(
    grid_x, grid_y, prop, table_in, rows_in, dft_in, out,
    staged, upper, lower, part, dens, weights, sent, table, rows, dft,
    load_sems, spin_sems, small_sems, send_sem, recv_sem,
):
    devices = out.shape[0]
    tiles = staged.shape[0]
    rows_x, width = staged.shape[-2:]
    pitch = upper.shape[1] // rows_x
    middle = weights.shape[1] // 2
    channels = table.shape[1]

    def load(t):
        return pltpu.make_async_copy(
            prop.at[:, :, :, :, pl.ds(t * width, width)], staged.at[t], load_sems.at[t]
        )

    def load_spin(spin):
        return pltpu.make_async_copy(
            prop.at[:, spin, :, :, pl.ds(0, width)], staged.at[0, :, spin], spin_sems.at[spin]
        )

    me_x, me_y = lax.axis_index("gx"), lax.axis_index("gy")
    me = me_x * grid_y + me_y
    if grid_y == 4:
        low = lax.rem(me_y, 2)
        other = 2 - (me_y - low)
        far, near = [other, other + 1], [me_y + 1 - 2 * low]
    else:
        far, near = [lax.rem(me_y + i, grid_y) for i in range(1, grid_y)], []

    urgent, lazy = far[: len(far) // 2], far[len(far) // 2 :]
    every = tuple(range(grid_x))

    def targets(columns, own):
        for i in every[own:]:
            for to_y in columns:
                yield (lax.rem(me_x + i, grid_x) if own else jnp.int32(i)), to_y

    def signal_all():
        @pl.loop(0, grid_x)
        def _(i):
            for to_y in far + near:
                signal(i, to_y)

        @pl.loop(1, grid_x)
        def _(i):
            signal(lax.rem(me_x + i, grid_x), me_y)

    def signal(x, y):
        pl.semaphore_signal(
            barrier, inc=1, device_id={"gx": x, "gy": y}, device_id_type=MESH
        )

    small = [
        pltpu.make_async_copy(source, target, small_sems.at[n])
        for n, (source, target) in enumerate(((table_in, table), (rows_in, rows), (dft_in, dft)))
    ]
    load_spin(0).start()
    small[0].start()
    small[1].start()
    for spin in range(1, SPINS):
        load_spin(spin).start()
    small[2].start()
    barrier = pltpu.get_barrier_semaphore()
    signal_all()
    slots = [(h, x) for h in range(PAIRED) for x in range(rows_x)]

    def first_products(t, ready=None):
        products(staged.at[t], 0, middle, upper, ready)

    def second_products(t):
        for h, x in slots:
            columns = upper[h, pl.ds(x * pitch, middle), :].astype(jnp.bfloat16)
            part[h, x] = jnp.dot(
                weights[:, :middle], columns, preferred_element_type=jnp.float32
            )
        products(staged.at[t], middle, 2 * middle, lower)

    def finish(t, slot):
        for h, x in slots:
            columns = lower[h, pl.ds(x * pitch, middle), :].astype(jnp.bfloat16)
            value = part[h, x] + jnp.dot(
                weights[:, middle:], columns, preferred_element_type=jnp.float32
            )
            dens[h, 0, pl.ds(x, channels, stride=rows_x), :] = value[:channels]
            dens[h, 1, pl.ds(x, channels, stride=rows_x), :] = value[channels:]
        left = jnp.concatenate(
            [jnp.concatenate([dens[h, 0], dens[h, 1]], axis=1) for h in range(PAIRED)], axis=0
        ).astype(jnp.bfloat16)
        value = lax.dot_general(
            dft[...], left, (((1,), (1,)), ((), ())), preferred_element_type=jnp.float32
        )
        pieces = [
            value[:, h * LANES : (h + 1) * LANES].reshape(devices, 2 * LANES // devices, LANES)
            for h in range(PAIRED)
        ]
        sent[:, slot] = jnp.concatenate(pieces, axis=1).astype(jnp.bfloat16)

    def push(columns, own, first, count=1):
        for x, y in targets(columns, own):
            pltpu.make_async_remote_copy(
                src_ref=sent.at[x * grid_y + y, pl.ds(first, count)],
                dst_ref=out.at[me, pl.ds(first, count)],
                send_sem=send_sem, recv_sem=recv_sem,
                device_id={"gx": x, "gy": y}, device_id_type=MESH,
            ).start()

    def ready(spin):
        load_spin(spin).wait()
        if spin == SPINS - 1:
            for t in range(1, tiles):
                load(t).start()

    first_products(0, ready)
    small[0].wait()
    small[1].wait()
    weights[...] = folded_weights(jnp.transpose(table[...]), rows[...])
    second_products(0)
    small[2].wait()
    finish(0, 0)
    pl.semaphore_wait(barrier, grid_x * grid_y - 1)
    push(urgent, 0, 0)
    push(lazy, 0, 0)
    last = tiles - 1
    for t in range(1, tiles):
        load(t).wait()
        if t > 1:
            finish(t - 1, t - 1)
        first_products(t)
        if t > 1:
            push(urgent, 0, t - 1)
            if t < last:
                push(lazy, 0, t - 1)
            if t == 2:
                push(near, 0, 0, 2)
                push([me_y], 1, 0, 2)
        second_products(t)
    finish(last, last)
    push(urgent, 0, last)
    push(near, 0, 2, tiles - 2)
    push([me_y], 1, 2, tiles - 2)
    push(lazy, 0, max(last - 1, 1), last - max(last - 1, 1) + 1)
    out[me] = sent[me]
    rest = sent.at[pl.ds(0, devices - 1)]
    pltpu.make_async_copy(rest, rest, recv_sem).wait()
    pltpu.make_async_copy(rest, rest, send_sem).wait()


def front(prop, gamma_table, devices, grid_y, extent):
    rows_x, sites = prop.shape[-2:]
    tiles = sites // (LANES * PAIRED)
    height = 2 * LANES // devices * PAIRED
    channels = gamma_table.shape[0]
    rows = np.zeros((8, len(ROWS)), np.int32)
    rows[:5] = np.array(ROWS, np.int32).T
    pinned = [
        pltpu.with_memory_space_constraint(array, pltpu.HBM)
        for array in (
            prop, gamma_table.T, jnp.asarray(rows), jnp.asarray(table_z(extent), jnp.bfloat16)
        )
    ]
    return pl.pallas_call(
        functools.partial(front_kernel, devices // grid_y, grid_y),
        out_shape=pltpu.VMEM((devices, tiles, height, LANES), jnp.bfloat16),
        in_specs=[pl.BlockSpec(memory_space=pltpu.HBM)] * 4,
        out_specs=pl.BlockSpec(memory_space=pltpu.VMEM),
        scratch_shapes=[
            pltpu.VMEM((tiles, *prop.shape[:-1], PAIRED * LANES), jnp.bfloat16),
            pltpu.VMEM((PAIRED, (len(ROWS) // 2 + PITCH) * rows_x, LANES), jnp.float32),
            pltpu.VMEM((PAIRED, (len(ROWS) // 2 + PITCH) * rows_x, LANES), jnp.float32),
            pltpu.VMEM((PAIRED, rows_x, 2 * channels, LANES), jnp.float32),
            pltpu.VMEM((PAIRED, 2, channels * rows_x, LANES), jnp.float32),
            pltpu.VMEM((2 * channels, len(ROWS)), jnp.bfloat16),
            pltpu.VMEM((devices, tiles, height, LANES), jnp.bfloat16),
            pltpu.VMEM(gamma_table.shape[::-1], jnp.int32),
            pltpu.VMEM(rows.shape, jnp.int32),
            pltpu.VMEM((2 * LANES, 2 * LANES), jnp.bfloat16),
            pltpu.SemaphoreType.DMA((tiles,)),
            pltpu.SemaphoreType.DMA((SPINS,)),
            pltpu.SemaphoreType.DMA((3,)),
            pltpu.SemaphoreType.DMA,
            pltpu.SemaphoreType.DMA,
        ],
        compiler_params=pltpu.CompilerParams(
            vmem_limit_bytes=60 * 1024 * 1024, collective_id=0, has_side_effects=True
        ),
    )(*pinned)


def back_kernel(blocks, along_y, along_x, out, mid, result, sem):
    grid_x, _, width = blocks.shape
    channels, local_k, extent, lanes = out.shape
    rows_x = width // channels
    cols = local_k * lanes
    for gx in range(grid_x):
        mid[gx] = lax.dot_general(
            blocks[gx], along_y[...], (((0,), (0,)), ((), ())), preferred_element_type=jnp.float32
        )
    for g in range(channels):
        value = mid[:, g * rows_x : (g + 1) * rows_x, :].reshape(grid_x * rows_x, 2 * cols)
        value = value.astype(jnp.bfloat16)
        stacked = jnp.concatenate([value[:, :cols], value[:, cols:]], axis=0)
        spectrum = jnp.dot(along_x[...], stacked, preferred_element_type=jnp.float32)
        for k in range(local_k):
            result[g, k] = spectrum[:, k * lanes : (k + 1) * lanes]
        pltpu.make_async_copy(result.at[g], out.at[g], sem).start()
    pltpu.make_async_copy(result, out, sem).wait()


def back(blocks, channels, extent, local_k):
    grid_x, _, width = blocks.shape
    vmem = pl.BlockSpec(memory_space=pltpu.VMEM)
    shape = (channels, local_k, extent, 2 * extent)
    return pl.pallas_call(
        back_kernel,
        out_shape=jax.ShapeDtypeStruct(shape, jnp.float32),
        in_specs=[vmem] * 3,
        out_specs=pl.BlockSpec(memory_space=pl.ANY),
        scratch_shapes=[
            pltpu.VMEM((grid_x, width, 4 * local_k * extent), jnp.float32),
            pltpu.VMEM(shape, jnp.float32),
            pltpu.SemaphoreType.DMA,
        ],
        compiler_params=pltpu.CompilerParams(vmem_limit_bytes=24 * 1024 * 1024),
    )(
        blocks,
        jnp.asarray(table_y(extent, local_k), jnp.bfloat16),
        jnp.asarray(table_x(extent), jnp.bfloat16),
    )


def body(propagator, gamma_table):
    slices, rows_x, sites = propagator.shape[0], propagator.shape[-2], propagator.shape[-1]
    grid_x, grid_y = lax.axis_size("gx"), lax.axis_size("gy")
    devices = grid_x * grid_y
    extent = grid_x * rows_x
    channels = gamma_table.shape[0]
    local_k = extent // devices
    results = []
    for t in range(slices):
        prop = propagator[t].reshape(2, SPINS, -1, rows_x, sites)
        blocks = front(prop, gamma_table, devices, grid_y, extent)
        blocks = blocks.reshape(grid_x, -1, LANES)
        results.append(back(blocks, channels, extent, local_k))
    return jnp.stack(results)


def solution(mesh):
    return jax.shard_map(
        body,
        mesh=mesh,
        in_specs=(P("ta", None, None, None, None, None, "gx", "gy"), P()),
        out_specs=P("ta", None, ("gx", "gy"), None, None),
        check_vma=False,
    )
```

```python
import functools
import math

import jax
import jax.numpy as jnp
import numpy as np
from jax import lax
from jax.experimental import pallas as pl
from jax.experimental.pallas import tpu as pltpu
from jax.sharding import PartitionSpec as P

LANES = 128
SPINS = 4
COLORS = 3
PITCH = 8
PAIRED = 2
MESH = pl.DeviceIdType.MESH


def pair_rows():
    rows = []
    for left in range(SPINS):
        for right in range(left, SPINS):
            for i in range(SPINS):
                for j in range(SPINS):
                    if left == right and i > j:
                        continue
                    if left == right and i == j:
                        rows.append((left, i, right, j, 2))
                    else:
                        rows.append((left, i, right, j, 0))
                        rows.append((left, i, right, j, 1))
    return rows


ROWS = pair_rows()
ROW_OF = {row: position for position, row in enumerate(ROWS)}


def dft_tables(length):
    index = np.arange(length)
    angles = (index[:, None] * index[None, :] % length) * (2.0 * math.pi / length)
    norm = 1.0 / math.sqrt(length)
    half = lambda v: (v * norm).astype(jnp.bfloat16).astype(np.float32)
    return half(np.cos(angles)), half(np.sin(angles))


def table_z(extent):
    cosine, sine = dft_tables(extent)
    per_tile = LANES // extent
    same = np.eye(per_tile, dtype=np.float32)
    block = np.zeros((extent, 2, per_tile, 2, per_tile, extent), np.float32)
    for c_out, c_in, values in ((0, 0, cosine), (0, 1, sine), (1, 0, -sine), (1, 1, cosine)):
        block[:, c_out, :, c_in] = np.einsum("zk,ab->kabz", values, same)
    return block.reshape(2 * LANES, 2 * LANES)


def table_y(extent, local_k):
    cosine, sine = dft_tables(extent)
    per_tile = LANES // extent
    groups = extent // per_tile
    block = np.zeros((groups, local_k, 2, per_tile, 2, local_k, 2, extent), np.float32)
    entries = (
        (0, 0, 0, cosine), (0, 0, 1, sine), (0, 1, 0, -sine), (0, 1, 1, cosine),
        (1, 0, 0, -sine), (1, 0, 1, cosine), (1, 1, 0, -cosine), (1, 1, 1, -sine),
    )
    for copy, c_out, c_in, values in entries:
        for k in range(local_k):
            block[:, k, c_in, :, copy, k, c_out] = values.reshape(groups, per_tile, extent)
    return block.reshape(groups * local_k * 2 * per_tile, 2 * local_k * 2 * extent)


def table_x(extent):
    cosine, sine = dft_tables(extent)
    return np.concatenate([cosine.T, sine.T], axis=1)


def folded_weights(table, rows):
    channels = table.shape[0]
    a1, a2, b1, b2, kind = (rows[i : i + 1, :] for i in range(5))

    def pick(spin, base):
        value = jnp.zeros((channels, rows.shape[1]), jnp.int32)
        for s in range(SPINS):
            value = jnp.where(spin == s, table[:, base + s : base + s + 1], value)
        return value

    def term(l1, l2, r1, r2):
        hit = (pick(r1, 0) == l1) & (pick(l2, 0) == r2)
        code = (pick(r1, SPINS) + pick(l2, SPINS)) & 3
        one = jnp.where(hit, 1.0, 0.0)
        real = jnp.where(code == 0, one, jnp.where(code == 2, -one, 0.0))
        imag = jnp.where(code == 1, one, jnp.where(code == 3, -one, 0.0))
        return real, imag

    fore_real, fore_imag = term(a1, a2, b1, b2)
    back_real, back_imag = term(b1, b2, a1, a2)
    sign = jnp.where(kind == 0, 1.0, jnp.where(kind == 1, -1.0, 0.0))
    real = fore_real + sign * back_real
    imag = fore_imag + sign * back_imag
    weight_real = jnp.where(kind == 1, -imag, real)
    weight_imag = jnp.where(kind == 1, real, imag)
    return jnp.concatenate([weight_real, weight_imag], axis=0).astype(jnp.bfloat16)


def component(s1, c1, s2, c2):
    return s1, (c1 * SPINS + s2) * COLORS + c2


def products(parts, first, last, rows_out, ready=None):
    rows_x = parts.shape[-2]
    pitch = rows_out.shape[1] // rows_x

    def put(row, value):
        value = value.astype(jnp.float32)
        place = pl.ds(ROW_OF[row] - first, rows_x, stride=pitch)
        for h in range(PAIRED):
            rows_out[h, place, :] = value[:, h * LANES : (h + 1) * LANES]

    for left in range(SPINS):
        for right in range(left, SPINS):
            at = [position for row, position in ROW_OF.items() if row[::2][:2] == (left, right)]
            if not first <= at[0] < last:
                continue
            if ready and left == 0:
                ready(right)
            for half in ((0, 1), (2, 3)):
                pairs = [(i, j) for i in half for j in range(SPINS) if left != right or i < j]
                diagonal = half if left == right else ()
                sums = {}
                for c1 in range(COLORS):
                    part = {}
                    for c2 in range(COLORS):
                        at_a = {i: component(left, c1, i, c2) for i in half}
                        at_b = {j: component(right, c1, j, c2) for _, j in pairs}
                        a = {i: (parts[0, *n], parts[1, *n]) for i, n in at_a.items()}
                        b = {j: (parts[0, *n], parts[1, *n]) for j, n in at_b.items()}
                        for i, j in pairs:
                            re = a[i][0] * b[j][0] + a[i][1] * b[j][1]
                            im = a[i][1] * b[j][0] - a[i][0] * b[j][1]
                            old = part.get((i, j))
                            part[i, j] = (re, im) if old is None else (old[0] + re, old[1] + im)
                        for i in diagonal:
                            wide = tuple(v.astype(jnp.float32) for v in a[i])
                            re = wide[0] * wide[0] + wide[1] * wide[1]
                            old = part.get(i)
                            part[i] = (re,) if old is None else (old[0] + re,)
                    for key, values in part.items():
                        old = sums.get(key)
                        sums[key] = values if old is None else tuple(o + v for o, v in zip(old, values))
                for i, j in pairs:
                    put((left, i, right, j, 0), sums[i, j][0])
                    put((left, i, right, j, 1), sums[i, j][1])
                for i in diagonal:
                    put((left, i, right, i, 2), sums[i][0])


def front_kernel(
    grid_x, grid_y, prop, table_in, rows_in, dft_in, out,
    staged, upper, lower, part, dens, weights, sent, table, rows, dft,
    load_sems, spin_sems, small_sems, send_sem, recv_sem,
):
    devices = out.shape[0]
    tiles = staged.shape[0]
    rows_x, width = staged.shape[-2:]
    pitch = upper.shape[1] // rows_x
    middle = weights.shape[1] // 2
    channels = table.shape[1]

    def load(t):
        return pltpu.make_async_copy(
            prop.at[:, :, :, :, pl.ds(t * width, width)], staged.at[t], load_sems.at[t]
        )

    def load_spin(spin):
        return pltpu.make_async_copy(
            prop.at[:, spin, :, :, pl.ds(0, width)], staged.at[0, :, spin], spin_sems.at[spin]
        )

    me_x, me_y = lax.axis_index("gx"), lax.axis_index("gy")
    me = me_x * grid_y + me_y
    if grid_y == 4:
        low = lax.rem(me_y, 2)
        other = 2 - (me_y - low)
        far, near = [other, other + 1], [me_y + 1 - 2 * low]
    else:
        far, near = [lax.rem(me_y + i, grid_y) for i in range(1, grid_y)], []

    urgent, lazy = far[: len(far) // 2], far[len(far) // 2 :]
    every = tuple(range(grid_x))
    early = me_y < grid_y // 2

    def targets(columns, own):
        for i in every[own:]:
            for to_y in columns:
                yield (lax.rem(me_x + i, grid_x) if own else jnp.int32(i)), to_y

    def signal_all():
        @pl.loop(0, grid_x)
        def _(i):
            for to_y in far + near:
                signal(i, to_y)

        @pl.loop(1, grid_x)
        def _(i):
            signal(lax.rem(me_x + i, grid_x), me_y)

    def signal(x, y):
        pl.semaphore_signal(
            barrier, inc=1, device_id={"gx": x, "gy": y}, device_id_type=MESH
        )

    small = [
        pltpu.make_async_copy(source, target, small_sems.at[n])
        for n, (source, target) in enumerate(((table_in, table), (rows_in, rows), (dft_in, dft)))
    ]
    small[0].start()
    small[1].start()
    for spin in range(SPINS):
        load_spin(spin).start()
    small[2].start()
    barrier = pltpu.get_barrier_semaphore()
    signal_all()
    slots = [(h, x) for h in range(PAIRED) for x in range(rows_x)]

    def first_products(t, ready=None):
        products(staged.at[t], 0, middle, upper, ready)

    def second_products(t):
        for h, x in slots:
            columns = upper[h, pl.ds(x * pitch, middle), :].astype(jnp.bfloat16)
            part[h, x] = jnp.dot(
                weights[:, :middle], columns, preferred_element_type=jnp.float32
            )
        products(staged.at[t], middle, 2 * middle, lower)

    def finish(t, slot):
        for h, x in slots:
            columns = lower[h, pl.ds(x * pitch, middle), :].astype(jnp.bfloat16)
            value = part[h, x] + jnp.dot(
                weights[:, middle:], columns, preferred_element_type=jnp.float32
            )
            dens[h, 0, pl.ds(x, channels, stride=rows_x), :] = value[:channels]
            dens[h, 1, pl.ds(x, channels, stride=rows_x), :] = value[channels:]
        left = jnp.concatenate(
            [jnp.concatenate([dens[h, 0], dens[h, 1]], axis=1) for h in range(PAIRED)], axis=0
        ).astype(jnp.bfloat16)
        value = lax.dot_general(
            dft[...], left, (((1,), (1,)), ((), ())), preferred_element_type=jnp.float32
        )
        pieces = [
            value[:, h * LANES : (h + 1) * LANES].reshape(devices, 2 * LANES // devices, LANES)
            for h in range(PAIRED)
        ]
        sent[:, slot] = jnp.concatenate(pieces, axis=1).astype(jnp.bfloat16)

    def push(columns, own, first, count=1):
        for x, y in targets(columns, own):
            pltpu.make_async_remote_copy(
                src_ref=sent.at[x * grid_y + y, pl.ds(first, count)],
                dst_ref=out.at[me, pl.ds(first, count)],
                send_sem=send_sem, recv_sem=recv_sem,
                device_id={"gx": x, "gy": y}, device_id_type=MESH,
            ).start()

    def ready(spin):
        load_spin(spin).wait()
        if spin == SPINS - 1:
            for t in range(1, tiles):
                load(t).start()

    small[0].wait()
    small[1].wait()
    weights[...] = folded_weights(jnp.transpose(table[...]), rows[...])
    first_products(0, ready)
    second_products(0)
    small[2].wait()
    finish(0, 0)
    pl.semaphore_wait(barrier, grid_x * grid_y - 1)
    def push_near(first, count):
        push(near, 0, first, count)
        push([me_y], 1, first, count)

    push(urgent, 0, 0)
    push(lazy, 0, 0)
    last = tiles - 1
    held = max(last - 1, 1)
    for t in range(1, tiles):
        load(t).wait()
        if t > 1:
            finish(t - 1, t - 1)
        first_products(t)
        if t > 1:
            if t == held:

                @pl.when(early)
                def _():
                    push_near(0, held)

            push(urgent, 0, t - 1)
            if t - 1 < held:
                push(lazy, 0, t - 1)
        second_products(t)
    finish(last, last)
    push(urgent, 0, last)

    @pl.when(early)
    def _():
        push_near(held, tiles - held)

    push(lazy, 0, held, tiles - held)

    @pl.when(jnp.logical_not(early))
    def _():
        push_near(0, tiles)

    out[me] = sent[me]
    rest = sent.at[pl.ds(0, devices - 1)]
    pltpu.make_async_copy(rest, rest, recv_sem).wait()
    pltpu.make_async_copy(rest, rest, send_sem).wait()


def front(prop, gamma_table, devices, grid_y, extent):
    rows_x, sites = prop.shape[-2:]
    tiles = sites // (LANES * PAIRED)
    height = 2 * LANES // devices * PAIRED
    channels = gamma_table.shape[0]
    rows = np.zeros((8, len(ROWS)), np.int32)
    rows[:5] = np.array(ROWS, np.int32).T
    pinned = [
        pltpu.with_memory_space_constraint(array, pltpu.HBM)
        for array in (
            prop, gamma_table.T, jnp.asarray(rows), jnp.asarray(table_z(extent), jnp.bfloat16)
        )
    ]
    return pl.pallas_call(
        functools.partial(front_kernel, devices // grid_y, grid_y),
        out_shape=pltpu.VMEM((devices, tiles, height, LANES), jnp.bfloat16),
        in_specs=[pl.BlockSpec(memory_space=pltpu.HBM)] * 4,
        out_specs=pl.BlockSpec(memory_space=pltpu.VMEM),
        scratch_shapes=[
            pltpu.VMEM((tiles, *prop.shape[:-1], PAIRED * LANES), jnp.bfloat16),
            pltpu.VMEM((PAIRED, (len(ROWS) // 2 + PITCH) * rows_x, LANES), jnp.float32),
            pltpu.VMEM((PAIRED, (len(ROWS) // 2 + PITCH) * rows_x, LANES), jnp.float32),
            pltpu.VMEM((PAIRED, rows_x, 2 * channels, LANES), jnp.float32),
            pltpu.VMEM((PAIRED, 2, channels * rows_x, LANES), jnp.float32),
            pltpu.VMEM((2 * channels, len(ROWS)), jnp.bfloat16),
            pltpu.VMEM((devices, tiles, height, LANES), jnp.bfloat16),
            pltpu.VMEM(gamma_table.shape[::-1], jnp.int32),
            pltpu.VMEM(rows.shape, jnp.int32),
            pltpu.VMEM((2 * LANES, 2 * LANES), jnp.bfloat16),
            pltpu.SemaphoreType.DMA((tiles,)),
            pltpu.SemaphoreType.DMA((SPINS,)),
            pltpu.SemaphoreType.DMA((3,)),
            pltpu.SemaphoreType.DMA,
            pltpu.SemaphoreType.DMA,
        ],
        compiler_params=pltpu.CompilerParams(
            vmem_limit_bytes=60 * 1024 * 1024, collective_id=0, has_side_effects=True
        ),
    )(*pinned)


def back_kernel(blocks, along_y, along_x, out, mid, result, sem):
    grid_x, _, width = blocks.shape
    channels, local_k, extent, lanes = out.shape
    rows_x = width // channels
    cols = local_k * lanes
    for gx in range(grid_x):
        mid[gx] = lax.dot_general(
            blocks[gx], along_y[...], (((0,), (0,)), ((), ())), preferred_element_type=jnp.float32
        )
    for g in range(channels):
        value = mid[:, g * rows_x : (g + 1) * rows_x, :].reshape(grid_x * rows_x, 2 * cols)
        value = value.astype(jnp.bfloat16)
        stacked = jnp.concatenate([value[:, :cols], value[:, cols:]], axis=0)
        spectrum = jnp.dot(along_x[...], stacked, preferred_element_type=jnp.float32)
        for k in range(local_k):
            result[g, k] = spectrum[:, k * lanes : (k + 1) * lanes]
        pltpu.make_async_copy(result.at[g], out.at[g], sem).start()
    pltpu.make_async_copy(result, out, sem).wait()


def back(blocks, channels, extent, local_k):
    grid_x, _, width = blocks.shape
    vmem = pl.BlockSpec(memory_space=pltpu.VMEM)
    shape = (channels, local_k, extent, 2 * extent)
    return pl.pallas_call(
        back_kernel,
        out_shape=jax.ShapeDtypeStruct(shape, jnp.float32),
        in_specs=[vmem] * 3,
        out_specs=pl.BlockSpec(memory_space=pl.ANY),
        scratch_shapes=[
            pltpu.VMEM((grid_x, width, 4 * local_k * extent), jnp.float32),
            pltpu.VMEM(shape, jnp.float32),
            pltpu.SemaphoreType.DMA,
        ],
        compiler_params=pltpu.CompilerParams(vmem_limit_bytes=24 * 1024 * 1024),
    )(
        blocks,
        jnp.asarray(table_y(extent, local_k), jnp.bfloat16),
        jnp.asarray(table_x(extent), jnp.bfloat16),
    )


def body(propagator, gamma_table):
    slices, rows_x, sites = propagator.shape[0], propagator.shape[-2], propagator.shape[-1]
    grid_x, grid_y = lax.axis_size("gx"), lax.axis_size("gy")
    devices = grid_x * grid_y
    extent = grid_x * rows_x
    channels = gamma_table.shape[0]
    local_k = extent // devices
    results = []
    for t in range(slices):
        prop = propagator[t].reshape(2, SPINS, -1, rows_x, sites)
        blocks = front(prop, gamma_table, devices, grid_y, extent)
        blocks = blocks.reshape(grid_x, -1, LANES)
        results.append(back(blocks, channels, extent, local_k))
    return jnp.stack(results)


def solution(mesh):
    return jax.shard_map(
        body,
        mesh=mesh,
        in_specs=(P("ta", None, None, None, None, None, "gx", "gy"), P()),
        out_specs=P("ta", None, ("gx", "gy"), None, None),
        check_vma=False,
    )
```
